256 devices in a mesh: seq: 16 (over z, core), head: 16 (over x, y).
Axes of the slice: x: 4, y: 4, z: 8, core: 2. Of those that a mesh axis runs over, the one named last changes fastest.
Arguments:
- grad_output: bfloat16 [16384, 4096], P('seq', 'head'), may hold values from -6 to 6
- out_weight: bfloat16 [4096, 8192], P('seq', 'head'), may hold values from -0.0625 to 0.0625
- ssd_out: bfloat16 [16384, 8192], P('seq', 'head'), may hold values from -520 to 520
- gate: bfloat16 [16384, 8192], P('seq', 'head'), may hold values from -5 to 5
- norm_weight: float32 [8192], P('head'), may hold values from 0.5 to 1.5
- time_step: float32 [128, 16384], P('head', 'seq'), may hold values from 0.01 to 0.1
- log_decay: float32 [128, 16384], P('head', 'seq'), may hold values from -0.7 to 0
- state_in: bfloat16 [16384, 8, 128], P('seq'), may hold values from -1.796875 to 1.796875
- state_out: bfloat16 [16384, 8, 128], P('seq'), may hold values from -1.796875 to 1.796875
- skip: float32 [128], P('head'), may hold values from 0.5 to 1.5
Outputs:
- grad_x: bfloat16 [16384, 8192], P('seq', 'head')
- grad_gate: bfloat16 [16384, 8192], P('seq', 'head')
- grad_out_weight: float32 [4096, 8192], P('seq', 'head')
The draws below stay inside these ranges and needn't reach their ends.
All inputs are finite; a program needn't handle non-finite values.
Results may differ from the reference program's by a relative error of at most 0.014.
Values may be sent and summed in bfloat16 or wider, within the bound.
No kernel may reach another device: no remote copies, remote signals or barrier semaphores. Data moves between devices by JAX's collectives and lax.ppermute only.
A program may use at most 128 MiB of HBM per device.

```python
import math
from functools import partial
import jax
import jax.numpy as jnp
from jax import lax

D = 4096
HEADS = 128
HDIM = 64
NSTATE = 128
GROUPS = 8
BLOCK_LEN = 256
TOK_DEV = 1024
TOKENS = 16384
DI = 8192


def draw_log_decay(key, part):
    keys = jax.random.split(jax.random.fold_in(key, 11), 7)
    order = jax.random.permutation(keys[0], HEADS)
    slow_count = HEADS // 2
    slow_heads = order < slow_count
    chain = float(TOKENS)
    slow_rate = jnp.exp(jax.random.uniform(keys[1], (HEADS,), jnp.float32, math.log(0.1 / chain), math.log(0.5 / chain)))
    fast_rate = jnp.exp(jax.random.uniform(keys[2], (HEADS,), jnp.float32, math.log(2.0 / chain), math.log(0.035)))
    fading_speed = jnp.where(slow_heads, slow_rate, fast_rate)
    blocks = TOKENS // TOK_DEV
    multiplier_coefficient = jnp.exp2(jax.random.uniform(keys[3], (HEADS, blocks), jnp.float32, -1.0, 1.0))
    multiplier_coefficient = jnp.repeat(multiplier_coefficient, TOK_DEV, axis=1)
    approximate_guess = jax.random.uniform(keys[4], (HEADS, TOKENS), jnp.float32, 0.5, 1.5)
    seat_locations = jax.random.randint(keys[5], (3,), 0, TOKENS)
    increment_lengths = jax.random.uniform(keys[6], (3,), jnp.float32, 0.22, 0.51)
    sequence_indices = jnp.arange(TOKENS)
    clustered_spans = jnp.max(jnp.where(sequence_indices[None, :] == seat_locations[:, None], increment_lengths[:, None], 0.0), axis=0)
    return (-(fading_speed[:, None] * multiplier_coefficient * approximate_guess) - clustered_spans[None, :]).astype(jnp.float32)


def draw_ssd_out(key, part):
    keys = jax.random.split(jax.random.fold_in(key, 23), 4)
    row_scale = jnp.exp(jax.random.uniform(keys[0], (TOKENS,), jnp.float32, 0.0, math.log(10.0)))
    column_scale = jnp.exp(jax.random.uniform(keys[1], (DI,), jnp.float32, math.log(0.3), math.log(3.0)))
    ramp = jnp.arange(DI, dtype=jnp.float32) / DI
    base = jax.random.truncated_normal(keys[3], -4.0, 4.0, (TOKENS, DI), jnp.float32)
    rising = jnp.power(3.0, 0.5 * ramp)
    return (base * row_scale[:, None] * (column_scale * rising)[None, :]).astype(jnp.bfloat16)


def spiked(entries, key, source, target, parts, factor):
    def block_of(dim):
        return (jnp.arange(entries.shape[dim]) // (entries.shape[dim] // parts)).reshape((-1,) + (1,) * (entries.ndim - 1 - dim))

    one_side = jax.random.permutation(key, parts)[block_of(target)]
    other_side = (block_of(target) + parts // 2) % parts
    return jnp.where((block_of(source) == one_side) | (block_of(source) == other_side), factor * entries, entries)


def block_scale(own_key, extent, pieces, low, high):
    def one(dim, blocks):
        steps = jax.random.uniform(jax.random.fold_in(jax.random.fold_in(own_key, 6), dim), (blocks,), jnp.float32, low / len(pieces), high / len(pieces))
        return jnp.repeat(jnp.exp(steps), extent[dim] // blocks).reshape((-1,) + (1,) * (len(extent) - dim - 1))

    level = one(*pieces[0])
    for cut in pieces[1:]:
        level = level * one(*cut)
    return level


def gaussian(own_key, shape, scale, most, shards=(), held_as=jnp.bfloat16):
    loudness = block_scale(own_key, shape, shards, -0.22, 0.18) if shards else 1.0
    drawn = jax.random.normal(own_key, shape, jnp.float32) * scale * loudness
    return jnp.minimum(jnp.maximum(drawn, -most), most).astype(held_as)


def heavy_noise(stream_key, extent, width, bound, cuts, heavy, kind=jnp.bfloat16):
    drawn = width * jax.random.normal(stream_key, extent, jnp.float32)
    if cuts:
        drawn = drawn * block_scale(stream_key, extent, cuts, -0.22, 0.18)
    return jnp.clip(spiked(drawn, jax.random.fold_in(stream_key, 3), *heavy), -bound, bound).astype(kind)


def setup_inputs(seed: int = 0) -> dict:
    seeds = jax.random.split(jax.random.key(seed), 11)
    return {
        "grad_output": heavy_noise(seeds[0], (TOKENS, D), 1.0, 6.0, ((0, 16), (1, 16)), (0, 1, 16, 2.0)),
        "out_weight": gaussian(seeds[1], (D, DI), DI ** -0.5, 0.0625, ((0, 16), (1, 16))),
        "ssd_out": draw_ssd_out(jax.random.fold_in(seeds[10], 71), 0),
        "gate": gaussian(seeds[3], (TOKENS, DI), 1.0, 5.0, ((0, 16), (1, 16))),
        "norm_weight": jnp.clip(1.0 + 0.1 * jax.random.normal(seeds[4], (DI,), jnp.float32), 0.5, 1.5),
        "time_step": jnp.clip(jnp.exp(math.log(0.1) - 2.3025851 * jax.random.uniform(seeds[5], (HEADS, TOKENS), jnp.float32) ** block_scale(seeds[5], (HEADS, TOKENS), ((0, 16), (1, 16)), -0.2, 0.2)), 0.01, 0.1),
        "log_decay": draw_log_decay(jax.random.fold_in(seeds[10], 71), 0),
        "state_in": gaussian(seeds[7], (TOKENS, GROUPS, NSTATE), 0.3, 1.796875, ((0, 16),)),
        "state_out": gaussian(seeds[8], (TOKENS, GROUPS, NSTATE), 0.3, 1.796875, ((0, 16),)),
        "skip": jnp.clip(0.5 + 1.0 * jax.random.uniform(seeds[9], (HEADS,), jnp.float32) ** block_scale(seeds[9], (HEADS,), ((0, 16),), -0.2, 0.2), 0.5, 1.5),
    }


epsilon = 1e-05

def head_grad(head, grad_ssd, time_step, log_decay, state_in, state_out, skip):
    group = (head // (HEADS // GROUPS)).astype(jnp.int32)
    blocks = TOKENS // BLOCK_LEN
    start_col = (head * HDIM).astype(jnp.int32)
    grad_cols = lax.dynamic_slice_in_dim(grad_ssd, start_col, HDIM, 1).astype(jnp.float32)
    grad_cols = grad_cols.reshape(blocks, BLOCK_LEN, HDIM)
    b_rows = lax.dynamic_index_in_dim(state_in, group, 1, keepdims=False).astype(jnp.float32)
    b_rows = b_rows.reshape(blocks, BLOCK_LEN, NSTATE)
    c_rows = lax.dynamic_index_in_dim(state_out, group, 1, keepdims=False).astype(jnp.float32)
    c_rows = c_rows.reshape(blocks, BLOCK_LEN, NSTATE)
    rates = lax.dynamic_index_in_dim(log_decay, head, 0, keepdims=False).reshape(blocks, BLOCK_LEN)
    step_sizes = lax.dynamic_index_in_dim(time_step, head, 0, keepdims=False).reshape(blocks, BLOCK_LEN)
    skip_head = lax.dynamic_index_in_dim(skip, head, 0, keepdims=False)
    cumulative = jnp.cumsum(rates, axis=1)
    block_total = cumulative[:, -1]
    sequence_indices = jnp.arange(BLOCK_LEN)
    upper_mask = sequence_indices[None, :] >= sequence_indices[:, None]
    scores = jnp.einsum('ktn,ksn->kts', b_rows, c_rows)
    log_gap = cumulative[:, None, :] - cumulative[:, :, None]
    block_weights = jnp.where(upper_mask, scores * jnp.exp(jnp.minimum(log_gap, 0.0)), 0.0).astype(jnp.bfloat16)
    block_weights = lax.optimization_barrier(block_weights).astype(jnp.float32)
    within = jnp.einsum('kts,ksp->ktp', block_weights, grad_cols)
    scaled = (jnp.exp(cumulative)[:, :, None] * grad_cols).astype(jnp.bfloat16)
    scaled = lax.optimization_barrier(scaled).astype(jnp.float32)
    block_state = jnp.einsum('ksp,ksn->kpn', scaled, c_rows)

    def fold_block(carried, inputs):
        state_now, total_now = inputs
        return (state_now + jnp.exp(total_now) * carried, carried)
    unused, carry = lax.scan(fold_block, jnp.zeros((HDIM, NSTATE), jnp.float32), (block_state, block_total), reverse=True)
    carry_low = lax.optimization_barrier(carry.astype(jnp.bfloat16)).astype(jnp.float32)
    across = jnp.einsum('kpn,ktn->ktp', carry_low, b_rows) * jnp.exp(block_total[:, None] - cumulative)[:, :, None]
    result = step_sizes[:, :, None] * (within + across) + skip_head * grad_cols
    return result.reshape(TOKENS, HDIM).astype(jnp.bfloat16)

def reference(grad_output, out_weight, ssd_out, gate, norm_weight, time_step, log_decay, state_in, state_out, skip):
    values = ssd_out.astype(jnp.float32)
    gate_values = gate.astype(jnp.float32)
    sigmoid_gate = jax.nn.sigmoid(gate_values)
    silu_gate = gate_values * sigmoid_gate
    gated_values = values * silu_gate
    inverse_rms = lax.rsqrt(lax.optimization_barrier(jnp.mean(gated_values * gated_values, axis=1, keepdims=True)) + epsilon)
    normed = (gated_values * inverse_rms * norm_weight).astype(jnp.bfloat16)
    normed_grad = jnp.dot(grad_output, out_weight, preferred_element_type=jnp.float32)
    weighted = lax.optimization_barrier(jnp.sum(norm_weight * normed_grad * gated_values, axis=1, keepdims=True))
    gated_grad = inverse_rms * norm_weight * normed_grad - gated_values * inverse_rms ** 3 * weighted / DI
    grad_gate = (gated_grad * values * sigmoid_gate * (1.0 + gate_values * (1.0 - sigmoid_gate))).astype(jnp.bfloat16)
    grad_ssd = (gated_grad * silu_gate).astype(jnp.bfloat16)
    grad_out_weight = jnp.dot(grad_output.T, normed, preferred_element_type=jnp.float32) * (1.0 / math.sqrt(TOKENS))
    per_head = lax.map(partial(head_grad, grad_ssd=grad_ssd, time_step=time_step, log_decay=log_decay, state_in=state_in, state_out=state_out, skip=skip), jnp.arange(HEADS, dtype=jnp.int32))
    grad_x = jnp.transpose(per_head, (1, 0, 2)).reshape(TOKENS, DI)
    return (grad_x, grad_gate, grad_out_weight)
```

```python
import functools
import math

import jax
import jax.numpy as jnp
from jax import lax
from jax.experimental import pallas as pl
from jax.experimental.pallas import tpu as pltpu
from jax.sharding import Mesh
from jax.sharding import PartitionSpec as P

HEADS = 128
GROUPS = 8
BLOCK = 256
HEAD = ("hx", "hy")
SEQ = ("sz", "sc")
EPS = 1e-05
F32 = jnp.float32
BF16 = jnp.bfloat16


def shift(x, axis, by):
    n = lax.axis_size(axis)
    return lax.ppermute(x, axis, [(i, (i + by) % n) for i in range(n)])


def from_later(x, axis, by):
    n = lax.axis_size(axis)
    return lax.ppermute(x, axis, [(i, i - by) for i in range(by, n)])


def sum_axis(x, axis):
    n = lax.axis_size(axis)
    parts = [shift(x, axis, k) for k in range(1, n)]
    total = x
    for part in parts:
        total = total + part
    return total


def ring_phase(block, axis):
    half = block.shape[0] // 2
    below = shift(block, axis, 1)
    above = shift(block, axis, -1)
    far_low = shift(below[:half], axis, 1)
    far_high = shift(above[half:], axis, -1)
    return below, above, far_low, far_high


def gather_colour(block, first, second):
    below, above, far_low, far_high = ring_phase(block, first)
    far = jnp.concatenate([far_low, far_high], axis=0)
    bundle = jnp.stack([block, below, above, far], axis=0)
    return (bundle,) + ring_phase(bundle, second)


OFFSETS = (0, -1, 1, 2)


def piece_heads(first_here, second_here, first_stride, second_stride):
    heads = []
    for second in OFFSETS:
        for first in OFFSETS:
            heads.append(
                lax.rem(first_here + first + 4, 4) * first_stride
                + lax.rem(second_here + second + 4, 4) * second_stride
            )
    return jnp.stack(heads).astype(jnp.int32)


def wide(col, width):
    return jnp.concatenate([col] * (width // col.shape[1]), axis=1)


def as_column(row):
    return jnp.transpose(jnp.broadcast_to(row, (128, row.shape[1])))


def row_sum(values):
    width = values.shape[1]
    narrow = values[:, :128]
    for k in range(1, width // 128):
        narrow = narrow + values[:, k * 128 : (k + 1) * 128]
    return jnp.sum(jnp.transpose(narrow), axis=0, keepdims=True)


def stats_kernel(y_ref, gate_ref, out_ref):
    gate = gate_ref[...].astype(F32)
    gated = y_ref[...].astype(F32) * (gate * jax.nn.sigmoid(gate))
    out_ref[...] = row_sum(gated * gated)


def norm_kernel(y_ref, gate_ref, nw_ref, sq_ref, out_ref, *, total):
    gate = gate_ref[...].astype(F32)
    gated = y_ref[...].astype(F32) * (gate * jax.nn.sigmoid(gate))
    inv = as_column(lax.rsqrt(sq_ref[...] / total + EPS))
    out_ref[...] = (gated * wide(inv, gated.shape[1]) * nw_ref[...]).astype(BF16)


def prep_kernel(ld_ref, dt_ref, b_ref, c_ref, spread_ref, bw_ref, ecum_ref, dec_ref, dte_ref):
    heads = ld_ref.shape[0]
    hi = lax.Precision.HIGHEST
    rows = lax.broadcasted_iota(jnp.int32, (BLOCK, BLOCK), 0)
    cols = lax.broadcasted_iota(jnp.int32, (BLOCK, BLOCK), 1)
    keep = cols >= rows
    cum = jnp.dot(ld_ref[...], keep.astype(F32), precision=hi, preferred_element_type=F32)
    total = cum[:, BLOCK - 1 : BLOCK]
    spread = spread_ref[...]

    def expand(x):
        return lax.dot_general(
            x, spread, (((0,), (0,)), ((), ())), precision=hi, preferred_element_type=F32
        )

    ecum_ref[...] = expand(jnp.exp(cum))
    dec_ref[...] = expand(dt_ref[...] * jnp.exp(total - cum))
    dte_ref[...] = expand(dt_ref[...])
    scores = lax.dot_general(
        b_ref[...], c_ref[...], (((1,), (1,)), ((), ())), preferred_element_type=F32
    )
    scores = jnp.where(keep, scores, 0.0)
    cum_t = jnp.transpose(cum)
    for h in range(heads):
        gap = cum[h : h + 1, :] - cum_t[:, h : h + 1]
        bw_ref[h] = (scores * jnp.exp(jnp.minimum(gap, 0.0))).astype(BF16)


def load_pieces(pieces, heads_ref, dest, sems, rows):
    copies = []
    at = 0
    for piece in pieces:
        for k in range(piece.shape[0]):
            col = pl.multiple_of(heads_ref[at] * 256, 256)
            copy = pltpu.make_async_copy(
                piece.at[k], dest.at[pl.ds(rows, piece.shape[1]), pl.ds(col, 256)], sems.at[at]
            )
            copy.start()
            copies.append(copy)
            at += 1
    return copies


def matmul_kernel(*refs):
    heads_a, heads_b = refs[0], refs[1]
    pieces = refs[2:12]
    w_ref, y_ref, gate_ref, nw_ref = refs[12:16]
    ng_ref, part_ref = refs[16:18]
    g_buf, w_buf, sem_a, sem_b, sem_w = refs[18:]
    w_copy = pltpu.make_async_copy(w_ref, w_buf, sem_w)
    copies_a = load_pieces(pieces[:5], heads_a, g_buf, sem_a, 0)
    w_copy.start()
    copies_b = load_pieces(pieces[5:], heads_b, g_buf, sem_b, 512)
    for copy in copies_a:
        copy.wait()
    w_copy.wait()
    for block in range(4):
        if block == 2:
            for copy in copies_b:
                copy.wait()
        rows = pl.ds(block * BLOCK, BLOCK)
        grad = jnp.dot(g_buf[rows, :], w_buf[...], preferred_element_type=F32)
        ng_ref[rows, :] = grad
        gate = gate_ref[rows, :].astype(F32)
        gated = y_ref[rows, :].astype(F32) * (gate * jax.nn.sigmoid(gate))
        part_ref[:, rows] = row_sum(nw_ref[...] * grad * gated)


def outer_kernel(parity_ref, heads_a, heads_b, *refs):
    pieces = refs[:10]
    normed_ref, out_ref, g_buf, sem_a, sem_b = refs[10:]
    copies = load_pieces(pieces[:5], heads_a, g_buf, sem_a, 0)
    copies += load_pieces(pieces[5:], heads_b, g_buf, sem_b, 512)
    for copy in copies:
        copy.wait()
    for k in range(out_ref.shape[0]):
        col = pl.multiple_of((2 * k + parity_ref[0]) * 256, 256)
        out_ref[k] = lax.dot_general(
            g_buf[:, pl.ds(col, 256)],
            normed_ref[...],
            (((0,), (0,)), ((), ())),
            preferred_element_type=F32,
        ).astype(BF16)


def gated_grad_of(ng_ref, y_ref, gate_ref, nw_ref, sq_ref, wt_ref, total):
    gate = gate_ref[...].astype(F32)
    values = y_ref[...].astype(F32)
    sig = jax.nn.sigmoid(gate)
    silu = gate * sig
    gated = values * silu
    inv = lax.rsqrt(sq_ref[...] / total + EPS)
    cube = as_column(inv * inv * inv * wt_ref[...] / total)
    width = gated.shape[1]
    grad = wide(as_column(inv), width) * nw_ref[...] * ng_ref[...] - gated * wide(cube, width)
    return grad, values, gate, sig, silu


def state_kernel(
    core_ref, etot_ref, ng_ref, y_ref, gate_ref, nw_ref, sq_ref, wt_ref, ecum_ref, c_ref,
    gs_ref, inside_ref, keep_ref, send_ref, carry, *, total
):
    step = pl.program_id(0)
    block = pl.num_programs(0) - 1 - step
    heads = carry.shape[0] // 64

    @pl.when(step == 0)
    def _():
        carry[...] = jnp.zeros_like(carry)

    grad, _, _, _, silu = gated_grad_of(ng_ref, y_ref, gate_ref, nw_ref, sq_ref, wt_ref, total)
    gs = (grad * silu).astype(BF16)
    gs_ref[...] = gs
    scaled = (ecum_ref[...] * gs.astype(F32)).astype(BF16)
    state = lax.dot_general(
        scaled, c_ref[...], (((0,), (0,)), ((), ())), preferred_element_type=F32
    )
    inside_ref[0] = carry[...]
    for h in range(heads):
        rows = slice(h * 64, (h + 1) * 64)
        carry[rows, :] = state[rows, :] + etot_ref[h, block] * carry[rows, :]

    @pl.when(block == 0)
    def _():
        half = carry.shape[0] // 2
        mine = pl.multiple_of(core_ref[0] * half, half)
        other = pl.multiple_of((1 - core_ref[0]) * half, half)
        keep_ref[...] = carry[pl.ds(mine, half), :]
        send_ref[...] = carry[pl.ds(other, half), :].astype(BF16)


def within_kernel(
    ng_ref, y_ref, gate_ref, nw_ref, sq_ref, wt_ref, gs_ref, bw_ref, dte_ref, skip_ref,
    gate_out_ref, part_ref, *, total
):
    grad, values, gate, sig, _ = gated_grad_of(
        ng_ref, y_ref, gate_ref, nw_ref, sq_ref, wt_ref, total
    )
    gate_out_ref[...] = (grad * values * sig * (1.0 + gate * (1.0 - sig))).astype(BF16)
    lane = lax.broadcasted_iota(jnp.int32, (BLOCK, 128), 1)
    for pair in range(bw_ref.shape[0] // 2):
        cols = slice(pair * 128, (pair + 1) * 128)
        gs = gs_ref[:, cols]
        low = jnp.where(lane < 64, gs, jnp.zeros_like(gs))
        high = jnp.where(lane < 64, jnp.zeros_like(gs), gs)
        inner = jnp.dot(bw_ref[2 * pair], low, preferred_element_type=F32)
        inner += jnp.dot(bw_ref[2 * pair + 1], high, preferred_element_type=F32)
        part_ref[:, cols] = dte_ref[:, cols] * inner + skip_ref[:, cols] * gs.astype(F32)


def final_kernel(
    core_ref, tail_ref, mine_ref, other_ref, inside_ref, b_ref, dec_ref, part_ref, out_ref, low
):
    block = pl.program_id(0)
    half = mine_ref.shape[0]
    per = half // 64
    for own in range(2):
        first = (core_ref[0] if own else 1 - core_ref[0]) * per
        for h in range(per):
            head = first + h
            rows = pl.ds(pl.multiple_of(head * 64, 64), 64)
            remote = (mine_ref if own else other_ref)[h * 64 : (h + 1) * 64, :].astype(F32)
            low[rows, :] = (inside_ref[0, rows, :] + tail_ref[head, block] * remote).astype(BF16)
    across = lax.dot_general(
        b_ref[...], low[...], (((1,), (1,)), ((), ())), preferred_element_type=F32
    )
    out_ref[...] = (part_ref[...] + dec_ref[...] * across).astype(BF16)


def params(*semantics):
    return pltpu.CompilerParams(dimension_semantics=semantics, vmem_limit_bytes=48 * 2**20)


SMEM = functools.partial(pl.BlockSpec, memory_space=pltpu.SMEM)
ANY = functools.partial(pl.BlockSpec, memory_space=pl.ANY)


def on_device(
    grad_output, out_weight, ssd_out, gate, norm_weight, time_step, log_decay, state_in,
    state_out, skip,
):
    tok, width = ssd_out.shape
    total = float(width * lax.axis_size(HEAD))
    heads = time_step.shape[0]
    blocks = tok // BLOCK
    x, y, core = lax.axis_index("hx"), lax.axis_index("hy"), lax.axis_index("sc")
    core_1 = core.astype(jnp.int32)[None]
    nw = norm_weight[None]
    S = jax.ShapeDtypeStruct
    tok_spec = pl.BlockSpec((BLOCK, width), lambda i: (i, 0))
    row_spec = pl.BlockSpec((1, BLOCK), lambda i: (0, i))
    one_spec = pl.BlockSpec((1, width), lambda i: (0, 0))
    state_spec = pl.BlockSpec((BLOCK, 128), lambda i: (i, 0))

    weights = lax.all_gather(out_weight, SEQ, axis=0, tiled=True)

    half = tok // 2
    colour_a = gather_colour(grad_output[:half], "hx", "hy")
    colour_b = gather_colour(grad_output[half:], "hy", "hx")
    heads_a = piece_heads(x, y, 4, 1)
    heads_b = piece_heads(y, x, 1, 4)
    pieces = colour_a + colour_b

    squares = pl.pallas_call(
        stats_kernel,
        grid=(blocks,),
        in_specs=[tok_spec, tok_spec],
        out_specs=row_spec,
        out_shape=S((1, tok), F32),
        compiler_params=params("arbitrary"),
        name="stats",
    )(ssd_out, gate)
    squares = sum_axis(sum_axis(squares, "hx"), "hy")

    group = (x * 4 + y) * heads // (HEADS // GROUPS)
    b_rows = lax.dynamic_index_in_dim(state_in, group, 1, keepdims=False)
    c_rows = lax.dynamic_index_in_dim(state_out, group, 1, keepdims=False)
    spread = (jnp.arange(width)[None, :] // 64 == jnp.arange(heads)[:, None]).astype(F32)
    head_row = pl.BlockSpec((heads, BLOCK), lambda i: (0, i))
    block_weights, ecum, dec, dte = pl.pallas_call(
        prep_kernel,
        grid=(blocks,),
        in_specs=[
            head_row, head_row, state_spec, state_spec,
            pl.BlockSpec((heads, width), lambda i: (0, 0)),
        ],
        out_specs=[
            pl.BlockSpec((heads, BLOCK, BLOCK), lambda i: (0, i, 0)), tok_spec, tok_spec, tok_spec,
        ],
        out_shape=[
            S((heads, tok, BLOCK), BF16), S((tok, width), F32), S((tok, width), F32),
            S((tok, width), F32),
        ],
        compiler_params=params("arbitrary"),
        name="prep",
    )(log_decay, time_step, b_rows, c_rows, spread)

    totals = jnp.sum(log_decay.reshape(heads, blocks, BLOCK), axis=2)
    etot = jnp.exp(totals)
    whole = jnp.sum(totals, axis=1)
    tail = jnp.exp(whole[:, None] - jnp.cumsum(totals, axis=1))
    log_all = lax.all_gather(jnp.broadcast_to(whole[:, None], (heads, 128)), SEQ)
    log_all = log_all[:, :, 0]

    normed = pl.pallas_call(
        functools.partial(norm_kernel, total=total),
        grid=(blocks,),
        in_specs=[tok_spec, tok_spec, one_spec, row_spec],
        out_specs=tok_spec,
        out_shape=S((tok, width), BF16),
        compiler_params=params("arbitrary"),
        name="norm",
    )(ssd_out, gate, nw, squares)

    vmem = pl.BlockSpec(memory_space=pltpu.VMEM)
    normed_grad, weighted = pl.pallas_call(
        matmul_kernel,
        in_specs=[SMEM(), SMEM()] + [ANY()] * 11 + [vmem] * 3,
        out_specs=[vmem, vmem],
        out_shape=[S((tok, width), F32), S((1, tok), F32)],
        scratch_shapes=[
            pltpu.VMEM((tok, 4096), BF16),
            pltpu.VMEM((4096, width), BF16),
            pltpu.SemaphoreType.DMA((16,)),
            pltpu.SemaphoreType.DMA((16,)),
            pltpu.SemaphoreType.DMA,
        ],
        compiler_params=pltpu.CompilerParams(vmem_limit_bytes=48 * 2**20),
        name="normed_grad",
    )(heads_a, heads_b, *pieces, weights, ssd_out, gate, nw)
    weighted = sum_axis(sum_axis(weighted, "hx"), "hy")

    def outer(parity, name):
        return pl.pallas_call(
            outer_kernel,
            in_specs=[SMEM()] * 3 + [ANY()] * 10 + [vmem],
            out_specs=vmem,
            out_shape=S((8, 256, width), BF16),
            scratch_shapes=[
                pltpu.VMEM((tok, 4096), BF16),
                pltpu.SemaphoreType.DMA((16,)),
                pltpu.SemaphoreType.DMA((16,)),
            ],
            compiler_params=pltpu.CompilerParams(vmem_limit_bytes=48 * 2**20),
            name=name,
        )(parity, heads_a, heads_b, *pieces, normed)

    sent = shift(outer(1 - core_1, "outer_send"), "sc", 1)
    kept = outer(core_1, "outer_keep")
    pair_sum = (kept.astype(F32) + sent.astype(F32)).astype(BF16).reshape(8 * 256, width)
    weight_sum = lax.psum_scatter(pair_sum, "sz", scatter_dimension=0, tiled=True).astype(F32)
    grad_out_weight = weight_sum * (1.0 / math.sqrt(tok * lax.axis_size(SEQ)))

    back_tok = pl.BlockSpec((BLOCK, width), lambda i: (blocks - 1 - i, 0))
    back_row = pl.BlockSpec((1, BLOCK), lambda i: (0, blocks - 1 - i))
    half_rows = heads * 64 // 2
    half_spec = pl.BlockSpec((half_rows, 128), lambda i: (0, 0))
    grad_ssd, inside, keep, send = pl.pallas_call(
        functools.partial(state_kernel, total=total),
        grid=(blocks,),
        in_specs=[
            SMEM(), SMEM(), back_tok, back_tok, back_tok, one_spec, back_row, back_row, back_tok,
            pl.BlockSpec((BLOCK, 128), lambda i: (blocks - 1 - i, 0)),
        ],
        out_specs=[
            back_tok, pl.BlockSpec((1, heads * 64, 128), lambda i: (blocks - 1 - i, 0, 0)),
            half_spec, half_spec,
        ],
        out_shape=[
            S((tok, width), BF16), S((blocks, heads * 64, 128), F32), S((half_rows, 128), F32),
            S((half_rows, 128), BF16),
        ],
        scratch_shapes=[pltpu.VMEM((heads * 64, 128), F32)],
        compiler_params=params("arbitrary"),
        name="states",
    )(core_1, etot, normed_grad, ssd_out, gate, nw, squares, weighted, ecum, c_rows)

    z = lax.axis_index("sz")
    nz = lax.axis_size("sz")
    got = shift(send, "sc", 1).astype(F32)
    log_half = lax.dynamic_slice_in_dim(log_all, core * (heads // 2), heads // 2, 1)
    log_half = log_half.reshape(nz, 2, heads // 2)
    here = lax.dynamic_index_in_dim(log_half, z, 0, keepdims=False)

    def rows_of(factor):
        return jnp.repeat(factor, 64)[:, None]

    first = core == 0
    earlier = jnp.where(first, keep, got)
    later = jnp.where(first, got, keep)
    chip = (earlier + rows_of(jnp.exp(here[0])) * later).astype(BF16)
    chip_logs = jnp.sum(log_half, axis=1)
    order = jnp.arange(nz)
    carry = jnp.zeros((half_rows, 128), F32)
    for k in range(1, nz):
        part = from_later(chip, "sz", k).astype(F32)
        between = (order > z) & (order < z + k)
        coef = jnp.exp(jnp.sum(jnp.where(between[:, None], chip_logs, 0.0), axis=0))
        carry = carry + rows_of(coef) * part
    to_first = later + rows_of(jnp.exp(here[1])) * carry
    mine = jnp.where(first, to_first, carry)
    theirs = jnp.where(first, carry, to_first).astype(BF16)
    other = shift(theirs, "sc", 1)

    grad_gate, part = pl.pallas_call(
        functools.partial(within_kernel, total=total),
        grid=(blocks,),
        in_specs=[
            tok_spec, tok_spec, tok_spec, one_spec, row_spec, row_spec, tok_spec,
            pl.BlockSpec((heads, BLOCK, BLOCK), lambda i: (0, i, 0)), tok_spec, one_spec,
        ],
        out_specs=[tok_spec, tok_spec],
        out_shape=[S((tok, width), BF16), S((tok, width), F32)],
        compiler_params=params("arbitrary"),
        name="within",
    )(
        normed_grad, ssd_out, gate, nw, squares, weighted, grad_ssd, block_weights, dte,
        jnp.repeat(skip, 64)[None],
    )

    grad_x = pl.pallas_call(
        final_kernel,
        grid=(blocks,),
        in_specs=[
            SMEM(), SMEM(), half_spec, half_spec,
            pl.BlockSpec((1, heads * 64, 128), lambda i: (i, 0, 0)), state_spec, tok_spec, tok_spec,
        ],
        out_specs=tok_spec,
        out_shape=S((tok, width), BF16),
        scratch_shapes=[pltpu.VMEM((heads * 64, 128), BF16)],
        compiler_params=params("arbitrary"),
        name="final",
    )(core_1, tail, mine, other, inside, b_rows, dec, part)
    return grad_x, grad_gate, grad_out_weight


def solution(mesh):
    finer = Mesh(mesh.devices.reshape(8, 2, 4, 4), ("sz", "sc", "hx", "hy"))
    return jax.shard_map(
        on_device,
        mesh=finer,
        in_specs=(
            P(SEQ, HEAD), P(SEQ, HEAD), P(SEQ, HEAD), P(SEQ, HEAD), P(HEAD), P(HEAD, SEQ),
            P(HEAD, SEQ), P(SEQ, None, None), P(SEQ, None, None), P(HEAD),
        ),
        out_specs=(P(SEQ, HEAD), P(SEQ, HEAD), P(SEQ, HEAD)),
        check_vma=False,
    )
```
